32 devices in a mesh: fsdp: 8 (over z, y), tensor: 4 (over x, core).
Axes of the slice: x: 2, y: 2, z: 4, core: 2. Of those that a mesh axis runs over, the one named last changes fastest.
Arguments:
- hidden_in: bfloat16 [8192, 2048], P(('fsdp', 'tensor')), may hold values from -6 to 6
- lengths: int32 [8], P('fsdp'), may hold values from 256 to 1024, as said below
- attn_gain: float32 [2048], replicated, may hold values from 0.5 to 2
- query_weight: bfloat16 [2048, 2048], P('fsdp', 'tensor'), may hold values from -0.125 to 0.125
- key_weight: bfloat16 [2048, 1024], P('fsdp', 'tensor'), may hold values from -0.125 to 0.125
- value_weight: bfloat16 [2048, 1024], P('fsdp', 'tensor'), may hold values from -0.125 to 0.125
- output_gate: bfloat16 [2048, 2048], P('fsdp', 'tensor'), may hold values from -0.125 to 0.125
- query_gain: float32 [128], replicated, may hold values from 0.5 to 2
- key_gain: float32 [128], replicated, may hold values from 0.5 to 2
- out_weight: bfloat16 [2048, 2048], P('tensor', 'fsdp'), may hold values from -3 to 3
- mlp_gain: float32 [2048], replicated, may hold values from 0.5 to 2
- gate_weight: bfloat16 [2048, 6144], P('fsdp', 'tensor'), may hold values from -0.125 to 0.125
- up_weight: bfloat16 [2048, 6144], P('fsdp', 'tensor'), may hold values from -0.125 to 0.125
- down_weight: bfloat16 [6144, 2048], P('tensor', 'fsdp'), may hold values from -0.15625 to 0.15625
- cotangent: bfloat16 [8192, 2048], P(('fsdp', 'tensor')), may hold values from -6 to 6
Outputs:
- output: bfloat16 [8192, 2048], P(('fsdp', 'tensor'))
- grad_hidden: float32 [8192, 2048], P(('fsdp', 'tensor'))
- grad_attn_gain: float32 [2048], replicated
- grad_query_weight: float32 [2048, 2048], P('fsdp', 'tensor')
- grad_key_weight: float32 [2048, 1024], P('fsdp', 'tensor')
- grad_value_weight: float32 [2048, 1024], P('fsdp', 'tensor')
- grad_output_gate: float32 [2048, 2048], P('fsdp', 'tensor')
- grad_query_gain: float32 [128], replicated
- grad_key_gain: float32 [128], replicated
- grad_out_weight: float32 [2048, 2048], P('tensor', 'fsdp')
- grad_mlp_gain: float32 [2048], replicated
- grad_gate_weight: float32 [2048, 6144], P('fsdp', 'tensor')
- grad_up_weight: float32 [2048, 6144], P('fsdp', 'tensor')
- grad_down_weight: float32 [6144, 2048], P('tensor', 'fsdp')
The draws below stay inside these ranges and needn't reach their ends.
Inputs may be any that keep to these rules, and one draw needn't show every extreme that they name: The first lengths[s] slots of sequence s hold real tokens, the rest padding; some sequence has all 1024 and some 1024 // 4.
All inputs are finite; a program needn't handle non-finite values.
Results may differ from the reference program's by a relative error of at most 0.019.
Values may be sent and summed in bfloat16 or wider, within the bound.
A program may use at most 192 MiB of HBM per device.

```python
import math
import jax
import jax.numpy as jnp
from jax import lax

D = 2048
HQ = 16
HK = 8
HD = 128
FF = 6144
SEQ_LEN = 1024
SEQS = 8
TOKENS = 8192


def draw_lengths(key, part):
    key_lens = jax.random.fold_in(key, 11)
    key_top = jax.random.fold_in(key, 12)
    key_low = jax.random.fold_in(key, 13)
    drawn = jax.random.randint(key_lens, (SEQS,), SEQ_LEN // 4, SEQ_LEN + 1)
    longest_at = jax.random.randint(key_top, (), 0, SEQS)
    shortest_at = (longest_at + 1 + jax.random.randint(key_low, (), 0, SEQS - 1)) % SEQS
    position = jnp.arange(SEQS)
    drawn = jnp.where(position == longest_at, SEQ_LEN, drawn)
    drawn = jnp.where(position == shortest_at, SEQ_LEN // 4, drawn)
    return drawn.astype(jnp.int32)


def block_levels(key, extent, shards, least, high):
    def one(dim, parts):
        steps = jax.random.uniform(jax.random.fold_in(jax.random.fold_in(key, 6), dim), (parts,), jnp.float32, least / len(shards), high / len(shards))
        return jnp.repeat(jnp.exp(steps), extent[dim] // parts).reshape((-1,) + (1,) * (len(extent) - dim - 1))

    level = one(*shards[0])
    for cut in shards[1:]:
        level = level * one(*cut)
    return level


def bell_draw(rng, shape, spread, reach, split=(), kind=jnp.bfloat16):
    values = spread * jax.random.normal(rng, shape, jnp.float32)
    if split:
        values = values * block_levels(rng, shape, split, -0.22, 0.18)
    return jnp.clip(values, -reach, reach).astype(kind)


def setup_inputs(seed: int = 0) -> dict:
    key_list = jax.random.split(jax.random.key(seed), 16)
    hidden_in = bell_draw(key_list[0], (TOKENS, D), 1.0, 6.0, ((0, 32),))
    lengths = draw_lengths(jax.random.fold_in(key_list[15], 71), 0)
    attn_gain = jnp.clip(jnp.exp(jax.random.uniform(key_list[2], (D,), jnp.float32, math.log(0.5), math.log(2.0))), 0.5, 2.0)
    query_weight = bell_draw(key_list[3], (D, HQ * HD), D ** -0.5, 0.125, ((0, 8), (1, 4)))
    key_weight = bell_draw(key_list[4], (D, HK * HD), D ** -0.5, 0.125, ((0, 8), (1, 4)))
    value_weight = bell_draw(key_list[5], (D, HK * HD), D ** -0.5, 0.125, ((0, 8), (1, 4)))
    output_gate = bell_draw(key_list[6], (D, HQ * HD), D ** -0.5, 0.125, ((0, 8), (1, 4)))
    query_gain = jnp.clip(jnp.exp(jax.random.uniform(key_list[7], (HD,), jnp.float32, math.log(0.5), math.log(2.0))), 0.5, 2.0)
    key_gain = jnp.clip(jnp.exp(jax.random.uniform(key_list[8], (HD,), jnp.float32, math.log(0.5), math.log(2.0))), 0.5, 2.0)
    out_weight = bell_draw(key_list[9], (HQ * HD, D), (max(HD // 32, 1)) ** -0.5, 3.0, ((0, 4), (1, 8)))
    mlp_gain = jnp.clip(jnp.exp(jax.random.uniform(key_list[10], (D,), jnp.float32, math.log(0.5), math.log(2.0))), 0.5, 2.0)
    gate_weight = bell_draw(key_list[11], (D, FF), D ** -0.5, 0.125, ((0, 8), (1, 4)))
    up_weight = bell_draw(key_list[12], (D, FF), D ** -0.5, 0.125, ((0, 8), (1, 4)))
    down_weight = bell_draw(key_list[13], (FF, D), (FF // 4) ** -0.5, 0.15625, ((0, 4), (1, 8)))
    cotangent = bell_draw(key_list[14], (TOKENS, D), 1.0, 6.0, ((0, 32),))
    return dict(hidden_in=hidden_in, lengths=lengths, attn_gain=attn_gain, query_weight=query_weight, key_weight=key_weight, value_weight=value_weight, output_gate=output_gate, query_gain=query_gain, key_gain=key_gain, out_weight=out_weight, mlp_gain=mlp_gain, gate_weight=gate_weight, up_weight=up_weight, down_weight=down_weight, cotangent=cotangent)


NORM_EPSILON = 1e-06
ROPE_THETA = 1000000.0
MASKED_LOGIT = -1e+30

@jax.custom_vjp
def low(v):
    return lax.optimization_barrier(v.astype(jnp.bfloat16)).astype(jnp.float32)

@jax.custom_vjp
def low_back(v):
    return v

def low_keep(v):
    return (low(v), None)

def low_pass(kept, grad):
    return (grad,)

def back_keep(v):
    return (v, None)

def back_low(kept, grad):
    return (low(grad),)
low.defvjp(low_keep, low_pass)
low_back.defvjp(back_keep, back_low)

def matmul(first_op, second_op):
    return jnp.dot(first_op, second_op, precision=lax.Precision.HIGHEST, preferred_element_type=jnp.float32)

def rms_scale(values, gain_vec):
    return values * lax.rsqrt(lax.optimization_barrier(jnp.mean(values * values, axis=-1, keepdims=True)) + NORM_EPSILON) * gain_vec

def rotate_half(values):
    half_width = values.shape[-1] // 2
    return jnp.concatenate([-values[..., half_width:], values[..., :half_width]], axis=-1)

def rope_tables(slot_count, head_size):
    half_width = head_size // 2
    inverse = ROPE_THETA ** (-(jnp.arange(half_width, dtype=jnp.float32) * 2.0 / head_size))
    angles = jnp.arange(slot_count, dtype=jnp.float32)[:, None] * inverse[None, :]
    cosine = jnp.concatenate([jnp.cos(angles), jnp.cos(angles)], axis=-1)
    sine_table = jnp.concatenate([jnp.sin(angles), jnp.sin(angles)], axis=-1)
    return (cosine[:, None, :], sine_table[:, None, :])

def rope_apply(values, cosine, sine_table):
    return values * cosine + rotate_half(values) * sine_table

def attend_sequence(inputs):
    queries, keys_in, values_in, length = inputs
    grouped = queries.reshape(SEQ_LEN, HK, HQ // HK, HD)
    scores = low_back(jnp.einsum('qkgd,skd->kgqs', grouped, keys_in, precision=lax.Precision.HIGHEST))
    row_index = jnp.arange(SEQ_LEN)[:, None]
    col_index = jnp.arange(SEQ_LEN)[None, :]
    allowed = (col_index <= row_index) & (col_index < length)
    logits = jnp.where(allowed, scores * HD ** (-0.5), MASKED_LOGIT)
    highest = lax.optimization_barrier(jnp.max(logits, axis=-1, keepdims=True))
    weights_raw = jnp.exp(logits - highest)
    probs = low(weights_raw / lax.optimization_barrier(jnp.sum(weights_raw, axis=-1, keepdims=True)))
    attended = low_back(jnp.einsum('kgqs,skd->qkgd', probs, values_in, precision=lax.Precision.HIGHEST))
    return attended.reshape(SEQ_LEN, HQ * HD)

def layer(hidden, attn_gain, query_weight, key_weight, value_weight, output_gate, query_gain, key_gain, out_weight, mlp_gain, gate_weight, up_weight, down_weight, lengths):
    cosine, sine_table = rope_tables(SEQ_LEN, HD)
    position = jnp.arange(SEQ_LEN)
    valid_rows = (position[None, :] < lengths[:, None]).astype(jnp.float32).reshape(SEQS * SEQ_LEN, 1)
    normed_one = low(rms_scale(hidden, attn_gain))
    query_raw = low_back(matmul(normed_one, query_weight)).reshape(SEQS, SEQ_LEN, HQ, HD)
    key_raw = low_back(matmul(normed_one, key_weight)).reshape(SEQS, SEQ_LEN, HK, HD)
    value_in = low(low_back(matmul(normed_one, value_weight))).reshape(SEQS, SEQ_LEN, HK, HD)
    gate_pre = low_back(matmul(normed_one, output_gate))
    query_rot = low(rope_apply(rms_scale(query_raw, query_gain), cosine, sine_table))
    key_rot = low(rope_apply(rms_scale(key_raw, key_gain), cosine, sine_table))
    attended = lax.map(jax.checkpoint(attend_sequence), (query_rot, key_rot, value_in, lengths))
    attended = attended.reshape(SEQS * SEQ_LEN, HQ * HD)
    gated_out = low(attended * jax.nn.sigmoid(gate_pre))
    middle = hidden + low_back(matmul(gated_out, out_weight))
    normed_two = low(rms_scale(middle, mlp_gain))
    ffn_gate = low_back(matmul(normed_two, gate_weight))
    ffn_up = low_back(matmul(normed_two, up_weight))
    ffn_mid = low(ffn_gate * jax.nn.sigmoid(ffn_gate) * ffn_up)
    return (middle + low_back(matmul(ffn_mid, down_weight))) * valid_rows

def reference(hidden_in, lengths, attn_gain, query_weight, key_weight, value_weight, output_gate, query_gain, key_gain, out_weight, mlp_gain, gate_weight, up_weight, down_weight, cotangent):
    floats = tuple((array_in.astype(jnp.float32) for array_in in (hidden_in, attn_gain, query_weight, key_weight, value_weight, output_gate, query_gain, key_gain, out_weight, mlp_gain, gate_weight, up_weight, down_weight)))

    def forward(*params):
        return layer(*params, lengths)
    result, pullback = jax.vjp(forward, *floats)
    grads = pullback(cotangent.astype(jnp.float32))
    return (result.astype(jnp.bfloat16), grads[0], grads[1], grads[2], grads[3], grads[4], grads[5], grads[6], grads[7], grads[8], grads[9], grads[10], grads[11], grads[12])
```

```python
import functools

import jax
import jax.numpy as jnp
from jax import lax
from jax.experimental import pallas as pl
from jax.experimental.pallas import tpu as pltpu
from jax.sharding import PartitionSpec as P

NORM_EPSILON = 1e-06
ROPE_THETA = 1000000.0
MASKED_LOGIT = -1e30
F32 = jnp.float32
BF16 = jnp.bfloat16


def matmul(first_op, second_op):
    return jnp.dot(first_op, second_op, preferred_element_type=F32)


def matmul_tn(first_op, second_op):
    return lax.dot_general(
        first_op, second_op, (((0,), (0,)), ((), ())), preferred_element_type=F32
    )


def matmul_nt(first_op, second_op):
    return lax.dot_general(
        first_op, second_op, (((1,), (1,)), ((), ())), preferred_element_type=F32
    )


def normalize(values):
    inv_root = lax.rsqrt(jnp.mean(values * values, axis=-1, keepdims=True) + NORM_EPSILON)
    return (values * inv_root, inv_root)


def norm_back(gradient, unit_rows, inv_root, gain_vec):
    scaled = gradient * gain_vec
    return inv_root * (scaled - unit_rows * jnp.mean(scaled * unit_rows, axis=-1, keepdims=True))


def rope_tables(slot_count, head_size):
    half_width = head_size // 2
    inverse = ROPE_THETA ** (-(jnp.arange(half_width, dtype=F32) * 2.0 / head_size))
    angles = jnp.arange(slot_count, dtype=F32)[:, None] * inverse[None, :]
    cosine, sine = jnp.cos(angles), jnp.sin(angles)
    return (
        jnp.concatenate([cosine, cosine], axis=-1),
        jnp.concatenate([-sine, sine], axis=-1),
    )


def turn(values, cosine, signed_sine):
    return values * cosine + pltpu.roll(values, values.shape[-1] // 2, 1) * signed_sine


def turn_back(values, cosine, signed_sine):
    return values * cosine - pltpu.roll(values, values.shape[-1] // 2, 1) * signed_sine


def allowed_mask(first_row, rows, cols, length):
    row = first_row + lax.broadcasted_iota(jnp.int32, (rows, cols), 0)
    col = lax.broadcasted_iota(jnp.int32, (rows, cols), 1)
    return (col <= row) & (col < length)


def attend_forward_kernel(
    rows, group, scale,
    scalars, q_ref, k_ref, g_ref, v_ref, cos_ref, sin_ref, qgain_ref, kgain_ref,
    attended_ref, gated_ref, lse_ref, keys, values,
):
    length, me = scalars[0], scalars[1]
    head = k_ref.shape[1]
    blocks = k_ref.shape[0] // rows

    def at(i):
        return pl.ds(pl.multiple_of(jnp.bitwise_xor(me, i) * rows, rows), rows)

    for i in range(blocks):
        slot = slice(i * rows, (i + 1) * rows)
        unit, _ = normalize(k_ref[at(i), :])
        keys[slot, :] = turn(unit * kgain_ref[...], cos_ref[slot, :], sin_ref[slot, :]).astype(BF16)
        values[slot, :] = v_ref[at(i), :].astype(BF16)
    for h in range(group):
        lanes = slice(h * head, (h + 1) * head)
        for i in range(blocks):
            slot, span = slice(i * rows, (i + 1) * rows), (i + 1) * rows
            unit, _ = normalize(q_ref[at(i), lanes])
            query = turn(unit * qgain_ref[...], cos_ref[slot, :], sin_ref[slot, :]).astype(BF16)
            scores = matmul_nt(query, keys[:span, :]) * scale
            logits = jnp.where(allowed_mask(i * rows, rows, span, length), scores, MASKED_LOGIT)
            highest = jnp.max(logits, axis=-1, keepdims=True)
            weights = jnp.exp(logits - highest)
            total = jnp.sum(weights, axis=-1, keepdims=True)
            probs = (weights * (1.0 / total)).astype(BF16)
            result = matmul(probs, values[:span, :])
            attended_ref[at(i), lanes] = result
            gated_ref[at(i), lanes] = (result * jax.nn.sigmoid(g_ref[at(i), lanes])).astype(BF16)
            lse_ref[at(i), lanes] = jnp.broadcast_to(highest + jnp.log(total), (rows, head))


def attend_backward_kernel(
    rows, group, scale,
    scalars, q_ref, k_ref, g_ref, v_ref, cos_ref, sin_ref, qgain_ref, kgain_ref,
    attended_ref, lse_ref, gated_grad_ref,
    qk_send_ref, gv_send_ref, qgain_part_ref, kgain_part_ref,
    keys, values, key_grad, value_grad,
):
    length, me = scalars[0], scalars[1]
    c = pl.program_id(0)
    kv_heads = pl.num_programs(0)
    head = k_ref.shape[1]
    blocks = k_ref.shape[0] // rows
    tail = kv_heads * group * head

    def at(i):
        return pl.ds(pl.multiple_of(jnp.bitwise_xor(me, i) * rows, rows), rows)

    @pl.when(c == 0)
    def _():
        qgain_part_ref[...] = jnp.zeros_like(qgain_part_ref)
        kgain_part_ref[...] = jnp.zeros_like(kgain_part_ref)

    for i in range(blocks):
        slot = slice(i * rows, (i + 1) * rows)
        unit, _ = normalize(k_ref[at(i), :])
        keys[slot, :] = turn(unit * kgain_ref[...], cos_ref[slot, :], sin_ref[slot, :]).astype(BF16)
        values[slot, :] = v_ref[at(i), :].astype(BF16)
    key_grad[...] = jnp.zeros_like(key_grad)
    value_grad[...] = jnp.zeros_like(value_grad)
    for h in range(group):
        lanes = slice(h * head, (h + 1) * head)
        out_lanes = pl.ds(pl.multiple_of((c * group + h) * head, head), head)
        for i in range(blocks):
            slot, span = slice(i * rows, (i + 1) * rows), (i + 1) * rows
            cosine, sine = cos_ref[slot, :], sin_ref[slot, :]
            unit, root = normalize(q_ref[at(i), lanes])
            query = turn(unit * qgain_ref[...], cosine, sine).astype(BF16)
            gated_grad = gated_grad_ref[at(i), lanes]
            gate_sig = jax.nn.sigmoid(g_ref[at(i), lanes])
            attended = attended_ref[at(i), lanes]
            through = gated_grad * gate_sig
            att_grad = through.astype(BF16)
            gv_send_ref[at(i), out_lanes] = (through * attended * (1.0 - gate_sig)).astype(BF16)
            scores = matmul_nt(query, keys[:span, :]) * scale
            logits = jnp.where(allowed_mask(i * rows, rows, span, length), scores, MASKED_LOGIT)
            soft = jnp.exp(logits - lse_ref[at(i), lanes][:, :1])
            prob_grad = matmul_nt(att_grad, values[:span, :])
            centre = jnp.sum(soft * prob_grad, axis=-1, keepdims=True)
            score_grad = (scale * soft * (prob_grad - centre)).astype(BF16)
            query_grad = matmul(score_grad, keys[:span, :])
            key_grad[:span, :] += matmul_tn(score_grad, query)
            value_grad[:span, :] += matmul_tn(soft.astype(BF16), att_grad)
            normed = turn_back(query_grad, cosine, sine)
            qgain_part_ref[...] += jnp.sum(normed * unit, axis=0, keepdims=True)
            qk_send_ref[at(i), out_lanes] = norm_back(normed, unit, root, qgain_ref[...]).astype(BF16)
    out_lanes = pl.ds(pl.multiple_of(tail + c * head, head), head)
    for i in range(blocks):
        slot = slice(i * rows, (i + 1) * rows)
        unit, root = normalize(k_ref[at(i), :])
        normed = turn_back(key_grad[slot, :], cos_ref[slot, :], sin_ref[slot, :])
        kgain_part_ref[...] += jnp.sum(normed * unit, axis=0, keepdims=True)
        qk_send_ref[at(i), out_lanes] = norm_back(normed, unit, root, kgain_ref[...]).astype(BF16)
        gv_send_ref[at(i), out_lanes] = value_grad[slot, :].astype(BF16)


def attention_specs(seq, group, kv_heads, head):
    wide = pl.BlockSpec((seq, group * head), lambda c, *_: (0, c))
    thin = pl.BlockSpec((seq, head), lambda c, *_: (0, group * kv_heads + c))
    table = pl.BlockSpec((seq, head), lambda c, *_: (0, 0))
    gain = pl.BlockSpec((1, head), lambda c, *_: (0, 0))
    return wide, thin, table, gain


def attend_forward(scalars, qk_raw, gv_raw, tables, gains, rows, group, kv_heads, head, scale):
    seq = qk_raw.shape[0]
    wide, thin, table, gain = attention_specs(seq, group, kv_heads, head)
    shape = (seq, kv_heads * group * head)
    return pl.pallas_call(
        functools.partial(attend_forward_kernel, rows, group, scale),
        grid_spec=pltpu.PrefetchScalarGridSpec(
            num_scalar_prefetch=1,
            grid=(kv_heads,),
            in_specs=[wide, thin, wide, thin, table, table, gain, gain],
            out_specs=[wide, wide, wide],
            scratch_shapes=[pltpu.VMEM((seq, head), BF16), pltpu.VMEM((seq, head), BF16)],
        ),
        out_shape=[
            jax.ShapeDtypeStruct(shape, F32),
            jax.ShapeDtypeStruct(shape, BF16),
            jax.ShapeDtypeStruct(shape, F32),
        ],
        compiler_params=pltpu.CompilerParams(vmem_limit_bytes=40 << 20),
        cost_estimate=pl.CostEstimate(
            flops=4 * seq * seq * head * group * kv_heads,
            bytes_accessed=16 * seq * head * group * kv_heads,
            transcendentals=seq * seq * group * kv_heads,
        ),
        name="attend_forward",
    )(scalars, qk_raw, qk_raw, gv_raw, gv_raw, *tables, *gains)


def attend_backward(
    scalars, qk_raw, gv_raw, tables, gains, attended, lse, gated_grad,
    rows, group, kv_heads, head, scale,
):
    seq = qk_raw.shape[0]
    wide, thin, table, gain = attention_specs(seq, group, kv_heads, head)
    shape = (seq, kv_heads * (group + 1) * head)
    whole = pl.BlockSpec(shape, lambda c, *_: (0, 0))
    return pl.pallas_call(
        functools.partial(attend_backward_kernel, rows, group, scale),
        grid_spec=pltpu.PrefetchScalarGridSpec(
            num_scalar_prefetch=1,
            grid=(kv_heads,),
            in_specs=[wide, thin, wide, thin, table, table, gain, gain, wide, wide, wide],
            out_specs=[whole, whole, gain, gain],
            scratch_shapes=[
                pltpu.VMEM((seq, head), BF16),
                pltpu.VMEM((seq, head), BF16),
                pltpu.VMEM((seq, head), F32),
                pltpu.VMEM((seq, head), F32),
            ],
        ),
        out_shape=[
            jax.ShapeDtypeStruct(shape, BF16),
            jax.ShapeDtypeStruct(shape, BF16),
            jax.ShapeDtypeStruct((1, head), F32),
            jax.ShapeDtypeStruct((1, head), F32),
        ],
        compiler_params=pltpu.CompilerParams(vmem_limit_bytes=48 << 20),
        cost_estimate=pl.CostEstimate(
            flops=10 * seq * seq * head * group * kv_heads,
            bytes_accessed=24 * seq * head * group * kv_heads,
            transcendentals=seq * seq * group * kv_heads,
        ),
        name="attend_backward",
    )(scalars, qk_raw, qk_raw, gv_raw, gv_raw, *tables, *gains, attended, lse, gated_grad)


class Ring:
    def __init__(self, count):
        self.count = count
        self.order = list(range(0, count, 2)) + list(range(1, count, 2))[::-1]
        self.place_of = [self.order.index(i) for i in range(count)]
        self.up = [(self.order[p], self.order[(p + 1) % count]) for p in range(count)]
        self.down = [(b, a) for a, b in self.up]
        me = lax.axis_index("fsdp")
        self.place = jnp.where(me % 2 == 0, me // 2, count - 1 - me // 2)

    def blocks(self, values):
        return jnp.split(values, self.count, axis=-1)

    def turned(self, blocks, start):
        whole = jnp.concatenate(blocks + blocks, axis=-1)
        width = blocks[0].shape[-1]
        return lax.dynamic_slice_in_dim(whole, start * width, self.count * width, axis=-1)

    def to_relative(self, values):
        b = self.blocks(values)
        b = [b[self.order[-k % self.count]] for k in range(self.count)]
        return self.turned(b, (self.count - self.place) % self.count)

    def to_natural(self, values):
        b = self.blocks(self.turned(self.blocks(values), self.place))
        return jnp.concatenate([b[-self.place_of[i] % self.count] for i in range(self.count)], axis=-1)

    def send_up(self, values):
        return lax.ppermute(values, "fsdp", self.up)

    def send_down(self, values):
        return lax.ppermute(values, "fsdp", self.down)

    def gather(self, first, second):
        firsts, seconds = [first], [second]
        for _ in range(self.count - 1):
            firsts.append(self.send_up(firsts[-1]))
            seconds.append(self.send_down(seconds[-1]))
        return firsts, [seconds[-r % self.count] for r in range(self.count)]

    def reduce(self, first_block, second_block):
        first = first_block(1 % self.count)
        second = second_block(-1 % self.count)
        for step in range(2, self.count + 1):
            first = first_block(step % self.count) + self.send_up(first.astype(BF16)).astype(F32)
            second = second_block(-step % self.count) + self.send_down(second.astype(BF16)).astype(F32)
        return first, second


def partner(values, distance, count):
    return lax.ppermute(values, "tensor", [(i, i ^ distance) for i in range(count)])


def rows_gather(values):
    across = partner(values, 2, 4)
    beside = partner(values, 1, 4)
    return jnp.concatenate([values, beside, across, partner(across, 1, 4)], axis=0)


def rows_scatter(block):
    far = block(2) + partner(block(3).astype(BF16), 1, 4).astype(F32)
    far = partner(far.astype(BF16), 2, 4).astype(F32)
    near = partner(block(1).astype(BF16), 1, 4).astype(F32)
    return (block(0) + near) + far


def total_over(values, axis, count):
    step = 1
    while step < count:
        values = values + lax.ppermute(values, axis, [(i, i ^ step) for i in range(count)])
        step *= 2
    return values


def body(
    fsdp_count,
    hidden_in,
    lengths,
    attn_gain,
    query_weight,
    key_weight,
    value_weight,
    output_gate,
    query_gain,
    key_gain,
    out_weight,
    mlp_gain,
    gate_weight,
    up_weight,
    down_weight,
    cotangent,
):
    rows = hidden_in.shape[0]
    length = lengths[0]
    head = query_gain.shape[0]
    kv_heads = key_weight.shape[1] // head
    group = query_weight.shape[1] // head // kv_heads
    width = kv_heads * group * head
    scale = head ** (-0.5)
    me = lax.axis_index("tensor")
    ring = Ring(fsdp_count)
    block_size = hidden_in.shape[1] // fsdp_count

    def col_block(values, r):
        return values[:, r * block_size : (r + 1) * block_size]

    def row_block(values, j):
        return values[j * rows : (j + 1) * rows]

    qk_list, gv_list = ring.gather(
        jnp.concatenate([query_weight, key_weight], axis=1),
        jnp.concatenate([output_gate, value_weight], axis=1),
    )
    qk_full, gv_full = jnp.concatenate(qk_list, axis=0), jnp.concatenate(gv_list, axis=0)
    half = out_weight.shape[0] // 2
    out_first, out_second = ring.gather(out_weight[:half], out_weight[half:])
    out_full = jnp.concatenate(
        [jnp.concatenate(out_first, axis=1), jnp.concatenate(out_second, axis=1)], axis=0
    )
    gate_list, up_list = ring.gather(gate_weight, up_weight)
    gate_full, up_full = jnp.concatenate(gate_list, axis=0), jnp.concatenate(up_list, axis=0)
    ffn_half = down_weight.shape[0] // 2
    down_first, down_second = ring.gather(down_weight[:ffn_half], down_weight[ffn_half:])
    down_full = jnp.concatenate(
        [jnp.concatenate(down_first, axis=1), jnp.concatenate(down_second, axis=1)], axis=0
    )

    position = me * rows + jnp.arange(rows)
    valid_rows = (position < length).astype(F32)[:, None]
    attn_gain = ring.to_relative(attn_gain[None])
    mlp_gain = ring.to_relative(mlp_gain[None])
    residual = ring.to_relative(hidden_in).astype(F32)
    grad_rows = ring.to_relative(cotangent).astype(F32) * valid_rows
    unit_one, root_one = normalize(residual)
    normed_one = rows_gather((unit_one * attn_gain).astype(BF16))
    branch_full = rows_gather(grad_rows.astype(BF16))
    seq = normed_one.shape[0]
    tables = rope_tables(seq, head)
    scalars = jnp.stack([length, me.astype(jnp.int32)])
    gains = (query_gain[None], key_gain[None])
    qk_raw = matmul(normed_one, qk_full)
    gv_raw = matmul(normed_one, gv_full)
    attended, gated_out, lse = attend_forward(
        scalars, qk_raw, gv_raw, tables, gains, rows, group, kv_heads, head, scale
    )
    middle = residual + rows_scatter(lambda j: matmul(row_block(gated_out, j), out_full))
    unit_two, root_two = normalize(middle)
    normed_two = rows_gather((unit_two * mlp_gain).astype(BF16))
    ffn_gate = matmul(normed_two, gate_full)
    ffn_up = matmul(normed_two, up_full)
    ffn_sig = jax.nn.sigmoid(ffn_gate)
    ffn_act = ffn_gate * ffn_sig
    ffn_mid = (ffn_act * ffn_up).astype(BF16)

    down_grads = ring.reduce(
        lambda r: matmul_tn(ffn_mid[:, :ffn_half], col_block(branch_full, r)),
        lambda r: matmul_tn(ffn_mid[:, ffn_half:], col_block(branch_full, r)),
    )
    mid_grad = matmul_nt(branch_full, down_full)
    gate_grad = (mid_grad * ffn_up * ffn_sig * (1.0 + ffn_gate * (1.0 - ffn_sig))).astype(BF16)
    up_grad = (mid_grad * ffn_act).astype(BF16)
    norm_two_grad = rows_scatter(
        lambda j: matmul_nt(row_block(gate_grad, j), gate_full)
        + matmul_nt(row_block(up_grad, j), up_full)
    )
    gate_w_grad, up_w_grad = ring.reduce(
        lambda r: matmul_tn(col_block(normed_two, r), gate_grad),
        lambda r: matmul_tn(col_block(normed_two, r), up_grad),
    )
    mlp_gain_part = jnp.sum(norm_two_grad * unit_two, axis=0, keepdims=True)
    middle_grad = grad_rows + norm_back(norm_two_grad, unit_two, root_two, mlp_gain)
    ffn_branch = rows_scatter(lambda j: matmul(row_block(ffn_mid, j), down_full))
    output = ((middle + ffn_branch) * valid_rows).astype(BF16)

    attn_full_grad = rows_gather(middle_grad.astype(BF16))
    gated_grad = matmul_nt(attn_full_grad, out_full)
    out_grads = ring.reduce(
        lambda r: matmul_tn(gated_out[:, :half], col_block(attn_full_grad, r)),
        lambda r: matmul_tn(gated_out[:, half:], col_block(attn_full_grad, r)),
    )
    qk_send, gv_send, query_gain_part, key_gain_part = attend_backward(
        scalars, qk_raw, gv_raw, tables, gains, attended, lse, gated_grad,
        rows, group, kv_heads, head, scale,
    )
    norm_one_grad = rows_scatter(
        lambda j: matmul_nt(row_block(qk_send, j), qk_full)
        + matmul_nt(row_block(gv_send, j), gv_full)
    )
    qk_grad, gv_grad = ring.reduce(
        lambda r: matmul_tn(col_block(normed_one, r), qk_send),
        lambda r: matmul_tn(col_block(normed_one, r), gv_send),
    )
    attn_gain_part = jnp.sum(norm_one_grad * unit_one, axis=0, keepdims=True)
    grad_hidden = middle_grad + norm_back(norm_one_grad, unit_one, root_one, attn_gain)

    parts = jnp.concatenate(
        [
            ring.to_natural(attn_gain_part),
            ring.to_natural(mlp_gain_part),
            query_gain_part,
            key_gain_part,
        ],
        axis=1,
    )
    parts = total_over(total_over(parts, "tensor", 4), "fsdp", fsdp_count)[0]
    features = hidden_in.shape[1]
    return (
        ring.to_natural(output),
        ring.to_natural(grad_hidden),
        parts[:features],
        qk_grad[:, :width],
        qk_grad[:, width:],
        gv_grad[:, width:],
        gv_grad[:, :width],
        parts[2 * features : 2 * features + head],
        parts[2 * features + head :],
        jnp.concatenate(out_grads, axis=0),
        parts[features : 2 * features],
        gate_w_grad,
        up_w_grad,
        jnp.concatenate(down_grads, axis=0),
    )


def solution(mesh):
    assert mesh.shape["tensor"] == 4
    weight, turned = P("fsdp", "tensor"), P("tensor", "fsdp")
    tokens, same = P(("fsdp", "tensor"), None), P()
    return jax.shard_map(
        functools.partial(body, mesh.shape["fsdp"]),
        mesh=mesh,
        in_specs=(
            tokens, P("fsdp"), same, weight, weight, weight, weight, same, same,
            turned, same, weight, weight, turned, tokens,
        ),
        out_specs=(
            tokens, tokens, same, weight, weight, weight, weight, same, same,
            turned, same, weight, weight, turned,
        ),
        check_vma=False,
    )
```
